32 devices in a mesh: dp: 2 (over x), sp: 16 (over y, z, core).
Axes of the slice: x: 2, y: 2, z: 4, core: 2. Of those that a mesh axis runs over, the one named last changes fastest.
Arguments:
- x: bfloat16 [4096, 16384], P(('dp', 'sp')), parts along dimension 0
- gain: bfloat16 [16384], replicated
- wq: bfloat16 [16384, 16384], replicated
- wk: bfloat16 [16384, 16384], replicated
- wv: bfloat16 [16384, 16384], replicated
- wo: bfloat16 [16384, 16384], replicated
Outputs:
- output: bfloat16 [4096, 16384], P(('dp', 'sp')), parts along dimension 0
There are 2 independent parts. The reference program is written for one: setup_inputs(seed, part) draws one part's arguments, and reference() takes and returns one part's arrays. A program takes and returns all parts, laid end to end along the dimension named above; an argument that names none is the same for every part.
All inputs are finite; a program needn't handle non-finite values.
Results may differ from the reference program's by a relative error of at most 0.012.
Values are sent between devices in bfloat16 or wider.
A program may use at most 4.75 GiB of HBM per device.

```python
import jax
import jax.numpy as jnp
from jax import lax

ROWS = 2048
D = 16384
HEADS = 128
KV_HEADS = 128
HEAD = 128
THETA = 10000


def setup_inputs(seed: int = 0, part: int = 0) -> dict:
    kx, kn, kq, kk, kv, ko = jax.random.split(jax.random.key(seed), 6)

    def weights(key, rows, columns):
        return jax.random.normal(key, (rows, columns), jnp.float32) * rows**-0.5

    drawn = {
        "x": jax.random.normal(jax.random.fold_in(kx, part), (ROWS, D), jnp.float32),
        "gain": 1 + 0.1 * jax.random.normal(kn, (D,), jnp.float32),
        "wq": 2 * weights(kq, D, HEADS * HEAD),
        "wk": 2 * weights(kk, D, KV_HEADS * HEAD),
        "wv": 4 * weights(kv, D, KV_HEADS * HEAD),
        "wo": weights(ko, HEADS * HEAD, D),
    }
    return {k: v.astype(jnp.bfloat16) for k, v in drawn.items()}


def normed(x, gain):
    wide = x.astype(jnp.float32)
    scale = lax.rsqrt(jnp.mean(wide * wide, -1, keepdims=True) + 1e-6)
    return (wide * scale * gain.astype(jnp.float32)).astype(jnp.bfloat16)


def turned(t, place, theta):
    half = t.shape[-1] // 2
    angle = place.astype(jnp.float32)[:, None] * theta ** (-jnp.arange(half, dtype=jnp.float32) / half)
    cos, sin = jnp.cos(angle)[:, None], jnp.sin(angle)[:, None]
    a, b = t[..., :half].astype(jnp.float32), t[..., half:].astype(jnp.float32)
    return jnp.concatenate([a * cos - b * sin, b * cos + a * sin], -1).astype(jnp.bfloat16)


def matmul(a, w):
    return jnp.dot(a, w, preferred_element_type=jnp.float32).astype(jnp.bfloat16)


def einsum(form, a, b):
    return jnp.einsum(form, a.astype(jnp.float32), b.astype(jnp.float32))


def attention(q, k, v):
    scores = einsum("tgsd,ugd->gstu", q, k) * q.shape[-1] ** -0.5
    token = jnp.arange(q.shape[0])
    scores = jnp.where(token[:, None] >= token, scores, -jnp.inf)
    weights = jax.nn.softmax(scores, -1).astype(jnp.bfloat16)
    return einsum("gstu,ugd->tgsd", weights, v).astype(jnp.bfloat16)


def reference(x, gain, wq, wk, wv, wo):
    a, place = normed(x, gain), jnp.arange(ROWS)
    q = turned(matmul(a, wq).reshape(ROWS, HEADS, HEAD), place, THETA).reshape(ROWS, KV_HEADS, -1, HEAD)
    k = turned(matmul(a, wk).reshape(ROWS, KV_HEADS, HEAD), place, THETA)
    v = matmul(a, wv).reshape(ROWS, KV_HEADS, HEAD)
    seen = attention(q, k, v).reshape(ROWS, HEADS * HEAD)
    return (x.astype(jnp.float32) + jnp.dot(seen, wo, preferred_element_type=jnp.float32)).astype(jnp.bfloat16)
```

```python
import functools

import jax
import jax.numpy as jnp
from jax import lax
from jax.experimental import pallas as pl
from jax.experimental.pallas import tpu as pltpu
from jax.sharding import PartitionSpec as P

HEAD = 128
THETA = 10000
NEG = -1e30
HIDDEN = 2 * NEG
LOG2E = 1.4426950408889634
VMEM = 67043328
CHIPS = 8
UNITS = 8
PAIR = 2
GROUPS = UNITS // PAIR
UNIT = CHIPS * HEAD
TK, TN, BUFS = 2048, 1024, 6
SLOTS = 4
CHUNK = 1024
BLOCK = 512
ORDER = (4, 2, 6, 3, 5, 1, 7)
ANY = pl.BlockSpec(memory_space=pl.ANY)
FULL = pl.BlockSpec(memory_space=pltpu.VMEM)
MESH = pl.DeviceIdType.MESH


def _dot(a, b, ca=1, cb=0):
    return lax.dot_general(a, b, (((ca,), (cb,)), ((), ())), preferred_element_type=jnp.float32)


def _layer(x_ref, gain_ref, wq_ref, wk_ref, wv_ref, wo_ref, cos_ref, sin_ref,
           y_ref, x_other_ref, qkv_ref, back_ref, back_other_ref,
           a_s, w_s, acc_s, out_s, qkv_s, top_s, mix_s, gap_s, o_s, seen_s, x_s, y_s,
           a_sem, x_out_sem, x_in_sem, w_sem, send_sem, recv_sem, local_sem, qkv_sem, o_sem, back_sem, pass_sem, passed_sem, seen_sem, x_sem, y_sem, y_in_sem):
    dp, me = lax.axis_index("dp"), lax.axis_index("sp")
    chip, core = lax.div(me, 2), lax.rem(me, 2)
    rows, depth = x_ref.shape
    span = 2 * rows
    wide = wq_ref.shape[1] // 2
    half = wo_ref.shape[1] // 2
    kt, nt = depth // TK, half // TN
    made = UNITS * 3 * kt
    total = made + 2 * GROUPS * nt
    mine, theirs = (pl.ds(pl.multiple_of(c * rows, rows), rows) for c in (core, 1 - core))
    partner = (dp, 2 * chip + 1 - core)

    def peer(chip):
        return dp, 2 * chip + core

    def remote(src, dst, send, recv, device):
        return pltpu.make_async_remote_copy(src_ref=src, dst_ref=dst, send_sem=send, recv_sem=recv, device_id=device, device_id_type=MESH)


    def fetch(g):
        slot = lax.rem(g, BUFS)
        tile, k = lax.div(g, kt), lax.rem(g, kt)
        u, i = lax.div(tile, 3), lax.rem(tile, 3)
        for j, w in enumerate((wq_ref, wk_ref, wv_ref)):

            @pl.when((g < made) & (i == j))
            def _():
                src = w.at[pl.ds(pl.multiple_of(k * TK, TK), TK), pl.ds(pl.multiple_of(core * wide + u * UNIT, UNIT), TN)]
                pltpu.make_async_copy(src, w_s.at[slot], w_sem.at[slot]).start()

        @pl.when(g >= made)
        def _():
            p, n = lax.div(g - made, nt), lax.rem(g - made, nt)
            side = lax.rem(core + lax.rem(p, 2), 2)
            row = side * wide + lax.div(p, 2) * (PAIR * UNIT)
            src = wo_ref.at[pl.ds(pl.multiple_of(row, TK), TK), pl.ds(pl.multiple_of(core * half + n * TN, TN), TN)]
            pltpu.make_async_copy(src, w_s.at[slot], w_sem.at[slot]).start()

    def fetched(g):
        slot = lax.rem(g, BUFS)
        pltpu.make_async_copy(wq_ref.at[pl.ds(0, TK), pl.ds(0, TN)], w_s.at[slot], w_sem.at[slot]).wait()
        return slot

    states = pltpu.make_async_copy(x_ref, a_s.at[mine], a_sem)
    states.start()
    for k in range(BUFS - 1):
        fetch(jnp.int32(k))
    gap_s[...] = lax.broadcasted_iota(jnp.int32, (BLOCK, BLOCK), 1) - lax.broadcasted_iota(jnp.int32, (BLOCK, BLOCK), 0)
    acc_s[...] = jnp.zeros_like(acc_s)

    barrier = pltpu.get_barrier_semaphore()
    for r in ORDER:
        pl.semaphore_signal(barrier, inc=1, device_id=peer(lax.rem(chip + r, CHIPS)), device_id_type=MESH)
    pl.semaphore_signal(barrier, inc=1, device_id=partner, device_id_type=MESH)
    pl.semaphore_wait(barrier, CHIPS)


    shared = [remote(x_ref, to, x_out_sem.at[i], x_in_sem.at[i], partner) for i, to in enumerate((a_s.at[mine], x_other_ref))]
    shared[0].start()

    def norm(part):
        def chunk(c):
            return pl.ds(pl.multiple_of(c * CHUNK, CHUNK), CHUNK)

        def squares(c, total):
            t = a_s[part, chunk(c)].astype(jnp.float32)
            t = t * t
            return total + sum(t[:, n : n + 128] for n in range(0, CHUNK, 128))

        total = lax.fori_loop(0, depth // CHUNK, squares, jnp.zeros((rows, 128), jnp.float32))
        scale = lax.rsqrt(jnp.sum(total, -1, keepdims=True) / depth + 1e-6)

        def turn(c, _):
            t = a_s[part, chunk(c)].astype(jnp.float32)
            a_s[part, chunk(c)] = (t * scale * gain_ref[:, chunk(c)].astype(jnp.float32)).astype(jnp.bfloat16)

        lax.fori_loop(0, depth // CHUNK, turn, None)

    states.wait()
    norm(mine)
    pltpu.make_async_copy(x_ref, a_s.at[theirs], x_in_sem.at[0]).wait()
    shared[1].start()
    norm(theirs)


    def sent(slot):
        for r in ORDER:
            pltpu.make_async_copy(out_s.at[slot, 0], out_s.at[slot, 0], send_sem.at[slot, r]).wait()

    def kept():
        pltpu.make_async_copy(out_s.at[0, 0], qkv_ref.at[0, pl.ds(0, 2)], local_sem).wait()

    def make(g, _):
        tile, k = lax.div(g, kt), lax.rem(g, kt)
        i, out, second = lax.rem(tile, 3), lax.rem(lax.div(tile, 2), SLOTS), lax.rem(tile, 2)

        fetch(g + BUFS - 1)
        slot = fetched(g)
        acc_s[:, :TN] += _dot(a_s[:, pl.ds(pl.multiple_of(k * TK, TK), TK)], w_s[slot])

        def send(src, dst):
            for r in ORDER:
                to = lax.rem(chip + r, CHIPS)
                remote(out_s.at[(out, to, *src)], qkv_ref.at[(chip, *dst)], send_sem.at[out, r], recv_sem.at[lax.div(tile, 3 * PAIR), r], peer(to)).start()

        @pl.when(k == kt - 1)
        def _():
            @pl.when((tile >= 2 * SLOTS) & (second == 0))
            def _():
                sent(out)

            @pl.when(i < 2)
            def _():
                for d in range(CHIPS):
                    t = acc_s[:, d * HEAD : (d + 1) * HEAD].astype(jnp.bfloat16).astype(jnp.float32)
                    t = t * cos_ref[...] + pltpu.roll(t, HEAD // 2, 1) * sin_ref[...]
                    out_s[out, d, second] = t.astype(jnp.bfloat16)

            @pl.when(i == 2)
            def _():
                for d in range(CHIPS):
                    out_s[out, d, second] = acc_s[:, d * HEAD : (d + 1) * HEAD].astype(jnp.bfloat16)

            acc_s[:, :TN] = jnp.zeros((span, TN), jnp.float32)

            @pl.when(tile < 2)
            def _():
                send((second,), (tile,))

            @pl.when(second == 1)
            def _():
                both = (pl.ds(tile - 1, 2),)

                @pl.when(tile > 2)
                def _():
                    send((), both)
                    kept()

                pltpu.make_async_copy(out_s.at[out, chip], qkv_ref.at[(chip, *both)], local_sem).start()

    lax.fori_loop(0, made, make, None)
    kept()


    scale = HEAD**-0.5
    e = scale * LOG2E
    take = BLOCK // span
    ones = jnp.ones((8, BLOCK), jnp.bfloat16)

    def back_kept():
        pltpu.make_async_copy(o_s.at[0, 0], back_ref.at[pl.ds(0, PAIR), 0], local_sem).wait()

    def attend(g, _):
        units = pl.ds(g * PAIR, PAIR)
        blocks = pl.ds(g * 3 * PAIR, 3 * PAIR)
        for r in ORDER:
            here = qkv_ref.at[lax.rem(chip + CHIPS - r, CHIPS), blocks]
            pltpu.make_async_copy(here, here, recv_sem.at[g, r]).wait()
        load = pltpu.make_async_copy(qkv_ref.at[:, blocks], qkv_s, qkv_sem)
        load.start()
        load.wait()

        def queries(iq, _):
            top_s[...] = jnp.full_like(top_s, NEG)
            mix_s[...] = jnp.zeros_like(mix_s)
            asked = pl.ds(iq * take, take)

            def block(j, masked):
                here = pl.ds(j * take, take)
                scores = [_dot(qkv_s[here, 3 * u + 1].reshape(BLOCK, HEAD), qkv_s[asked, 3 * u].reshape(BLOCK, HEAD), 1, 1) for u in range(PAIR)]
                weights, keeps = [], []
                for u, s in enumerate(scores):
                    if masked:
                        s = jnp.where(gap_s[...] >= 0, s, HIDDEN)
                    old = top_s[u : u + 1, :]
                    top = jnp.maximum(old, s.max(axis=0, keepdims=True))
                    top_s[u : u + 1, :] = top
                    weights.append(jnp.exp2((s - top) * e).astype(jnp.bfloat16))
                    keeps.append(jnp.exp2((old - top) * e))
                for u, (p, keep) in enumerate(zip(weights, keeps)):
                    values = jnp.concatenate([qkv_s[here, 3 * u + 2].reshape(BLOCK, HEAD).T, ones], axis=0)
                    mix_s[u] = mix_s[u] * keep + _dot(values, p, 1, 0)

            lax.fori_loop(0, iq, lambda j, _: block(j, False), None)
            block(iq, True)

            for c in range(take):
                to = take * iq + c

                @pl.when((g > 0) & (to != chip))
                def _():
                    pltpu.make_async_copy(o_s.at[iq, c], o_s.at[iq, c], o_sem.at[iq, c]).wait()

            for u in range(PAIR):
                out = (mix_s[u, :HEAD, :] * (1 / mix_s[u, HEAD : HEAD + 1, :])).T
                o_s[iq, :, u] = out.reshape(take, span, HEAD).astype(jnp.bfloat16)

            for c in range(take):
                to = take * iq + c

                @pl.when(to != chip)
                def _():
                    r = lax.rem(to + CHIPS - chip, CHIPS)
                    remote(o_s.at[iq, c], back_ref.at[units, chip], o_sem.at[iq, c], back_sem.at[g, r], peer(to)).start()

                @pl.when(to == chip)
                def _():
                    pltpu.make_async_copy(o_s.at[iq, c], back_ref.at[units, chip], local_sem).start()

        lax.fori_loop(0, CHIPS // take, queries, None)
        back_kept()

    lax.fori_loop(0, GROUPS, attend, None)


    def arrived(g):
        units = pl.ds(g * PAIR, PAIR)
        for r in ORDER:
            here = back_ref.at[units, lax.rem(chip + CHIPS - r, CHIPS)]
            pltpu.make_async_copy(here, here, back_sem.at[g, r]).wait()
        remote(back_ref.at[units], back_other_ref.at[units], pass_sem.at[g], passed_sem.at[g], partner).start()
        pltpu.make_async_copy(back_ref.at[units], seen_s.at[0], seen_sem.at[0]).start()

    def handed(g):
        units = pl.ds(g * PAIR, PAIR)
        here = back_other_ref.at[units]
        pltpu.make_async_copy(here, here, passed_sem.at[g]).wait()
        pltpu.make_async_copy(here, seen_s.at[1], seen_sem.at[1]).start()

    def columns(n):
        return pl.ds(pl.multiple_of(core * half + n * TN, TN), TN)

    def residual(n):
        side = lax.rem(n, 2)
        return (pltpu.make_async_copy(x_ref.at[:, columns(n)], x_s.at[side, 0], x_sem.at[side, 0]),
                pltpu.make_async_copy(x_other_ref.at[:, columns(n)], x_s.at[side, 1], x_sem.at[side, 1]))

    def result(n):
        side = lax.rem(n, 2)
        return (pltpu.make_async_copy(y_s.at[side, 0], y_ref.at[:, columns(n)], y_sem.at[side, 0]),
                remote(y_s.at[side, 1], y_ref.at[:, columns(n)], y_sem.at[side, 1], y_in_sem, partner))

    def written(n):
        to_own, to_other = result(n)
        to_own.wait()
        to_other.wait_send()

    acc_s[...] = jnp.zeros_like(acc_s)
    pltpu.make_async_copy(x_ref, x_other_ref, x_in_sem.at[1]).wait()
    arrived(0)

    def project(t, _):
        p, n = lax.div(t, nt), lax.rem(t, nt)
        g, away = lax.div(p, 2), lax.rem(p, 2)
        final = p == 2 * GROUPS - 1

        @pl.when(made + t + BUFS - 1 < total)
        def _():
            fetch(made + t + BUFS - 1)

        @pl.when(n == 0)
        def _():
            here = back_ref.at[pl.ds(0, PAIR)]
            pltpu.make_async_copy(here, seen_s.at[away], seen_sem.at[away]).wait()

        @pl.when((n == nt - 2) & (away == 0))
        def _():
            handed(g)

        @pl.when((n == nt - 2) & (away == 1) & (g + 1 < GROUPS))
        def _():
            arrived(g + 1)

        @pl.when(final & (n == 0))
        def _():
            for c in residual(n):
                c.start()

        slot = fetched(made + t)
        left = jnp.concatenate([seen_s[away, u, s] for u in range(PAIR) for s in range(CHIPS)], axis=1)
        cols = pl.ds(pl.multiple_of(n * TN, TN), TN)
        acc_s[:, cols] += _dot(left, w_s[slot])

        @pl.when(final)
        def _():
            side = lax.rem(n, 2)

            @pl.when(n + 1 < nt)
            def _():
                for c in residual(n + 1):
                    c.start()

            @pl.when(n >= 2)
            def _():
                written(n - 2)

            for c in residual(n):
                c.wait()
            for i, part in enumerate((mine, theirs)):
                y_s[side, i] = (x_s[side, i].astype(jnp.float32) + acc_s[part, cols]).astype(jnp.bfloat16)
            for c in result(n):
                c.start()

    lax.fori_loop(0, 2 * GROUPS * nt, project, None)


    for n in range(max(nt - 2, 0), nt):
        written(jnp.int32(n))
    here = y_ref.at[:, pl.ds(pl.multiple_of((1 - core) * half, TN), half)]
    pltpu.make_async_copy(here, here, y_in_sem).wait()
    for slot in range(SLOTS):
        sent(slot)
    for i in range(2):
        pltpu.make_async_copy(x_ref, x_other_ref, x_out_sem.at[i]).wait()
    for iq in range(CHIPS // take):
        for c in range(take):

            @pl.when(take * iq + c != chip)
            def _():
                pltpu.make_async_copy(o_s.at[iq, c], o_s.at[iq, c], o_sem.at[iq, c]).wait()

    for g in range(GROUPS):
        here = back_ref.at[pl.ds(g * PAIR, PAIR)]
        pltpu.make_async_copy(here, here, pass_sem.at[g]).wait()


def layer(x, gain, wq, wk, wv, wo, cos, sin):
    rows, d = x.shape
    span, half = 2 * rows, wo.shape[1] // 2
    low, f32, dma = jnp.bfloat16, jnp.float32, pltpu.SemaphoreType.DMA
    blocks = CHIPS // (BLOCK // span)
    return pl.pallas_call(
        _layer,
        in_specs=[ANY, FULL] + [ANY] * 4 + [FULL] * 2,
        out_specs=[ANY] * 5,
        out_shape=[
            jax.ShapeDtypeStruct((rows, wo.shape[1]), low),
            jax.ShapeDtypeStruct((rows, d), low),
            jax.ShapeDtypeStruct((CHIPS, 3 * UNITS, span, HEAD), low),
            jax.ShapeDtypeStruct((UNITS, CHIPS, span, HEAD), low),
            jax.ShapeDtypeStruct((UNITS, CHIPS, span, HEAD), low),
        ],
        scratch_shapes=[
            pltpu.VMEM((span, d), low),
            pltpu.VMEM((BUFS, TK, TN), low),
            pltpu.VMEM((span, half), f32),
            pltpu.VMEM((SLOTS, CHIPS, 2, span, HEAD), low),
            pltpu.VMEM((CHIPS, 3 * PAIR, span, HEAD), low),
            pltpu.VMEM((PAIR, BLOCK), f32),
            pltpu.VMEM((PAIR, HEAD + 8, BLOCK), f32),
            pltpu.VMEM((BLOCK, BLOCK), jnp.int32),
            pltpu.VMEM((blocks, BLOCK // span, PAIR, span, HEAD), low),
            pltpu.VMEM((2, PAIR, CHIPS, span, HEAD), low),
            pltpu.VMEM((2, 2, rows, TN), low),
            pltpu.VMEM((2, 2, rows, TN), low),
            dma,
            dma((2,)),
            dma((2,)),
            dma((BUFS,)),
            dma((SLOTS, CHIPS)),
            dma((GROUPS, CHIPS)),
            dma,
            dma,
            dma((blocks, BLOCK // span)),
            dma((GROUPS, CHIPS)),
            dma((GROUPS,)),
            dma((GROUPS,)),
            dma((2,)),
            dma((2, 2)),
            dma((2, 2)),
            dma,
        ],
        compiler_params=pltpu.CompilerParams(vmem_limit_bytes=VMEM, collective_id=0, has_side_effects=True),
        cost_estimate=pl.CostEstimate(flops=16 * span * d * d // 4, bytes_accessed=4 * d * d, transcendentals=0),
        name="layer",
    )(x, gain.reshape(1, d), wq, wk, wv, wo, cos, sin)[0]


def solution(mesh):
    def step(x, gain, wq, wk, wv, wo):
        rows = x.shape[0]
        half = HEAD // 2
        place = lax.div(lax.axis_index("sp"), 2) * (2 * rows) + jnp.arange(2 * rows)
        angle = place.astype(jnp.float32)[:, None] * THETA ** (-jnp.arange(half, dtype=jnp.float32) / half)
        cos, sin = jnp.cos(angle), jnp.sin(angle)
        cos, sin = jnp.concatenate([cos, cos], 1), jnp.concatenate([-sin, sin], 1)
        return layer(x, gain, wq, wk, wv, wo, cos, sin)

    tokens, whole = P(("dp", "sp"), None), P(None, None)
    return jax.shard_map(
        step,
        mesh=mesh,
        in_specs=(tokens, P(None), whole, whole, whole, whole),
        out_specs=tokens,
        check_vma=False,
    )
```
